32 devices in a mesh: blk: 2 (over y), uly: 4 (over x, core), dp: 4 (over z).
Axes of the slice: x: 2, y: 2, z: 4, core: 2. Of those that a mesh axis runs over, the one named last changes fastest.
Arguments:
- tokens: bfloat16 [1024, 4096], P(('uly', 'dp')), may hold values from -6 to 6
- expert_ids: int32 [1024, 8], P(('uly', 'dp')), may hold values from 0 to 15, all different within a row; in each aligned block of 64 rows (0 to 63, 64 to 127, ...) at most 40 rows name the same one
- route_weight: float32 [1024, 8], P(('uly', 'dp')), may hold values from 0.05 to 0.5
- w_gate: bfloat16 [16, 4096, 1024], P(('uly', 'dp'), None, 'blk'), may hold values from -0.09375 to 0.09375
- w_up: bfloat16 [16, 4096, 1024], P(('uly', 'dp'), None, 'blk'), may hold values from -0.09375 to 0.09375
- w_down: bfloat16 [16, 1024, 4096], P(('uly', 'dp'), 'blk'), may hold values from -0.1875 to 0.1875
Outputs:
- mixed: bfloat16 [1024, 4096], P(('uly', 'dp'), 'blk')
The draws below stay inside these ranges and needn't reach their ends.
Inputs may be any that keep to these rules, and one draw needn't show every extreme that they name: `expert_ids`: each row names 8 different experts. In each aligned block of 64 rows (the rows of one device) no expert is named by more than 40 rows, and in some block one expert is named by exactly 40 rows.
All inputs are finite; a program needn't handle non-finite values.
Results may differ from the reference program's by a relative error of at most 0.015.
Values may be sent and summed in bfloat16 or wider, within the bound.
A program may use at most 64 MiB of HBM per device.

```python
import math
import jax
import jax.numpy as jnp
import numpy as np
from jax import lax

D = 4096
FF = 1024
TOPK = 8
TOK_DEV = 64
EXPERTS = 16
CAP = 40
TOKENS = 1024
N_BLK = 2
N_ULY = 4
N_DP = 4


def levels(own_key, shape, shards, least, largest):
    def one(axis_at, shards_of):
        heights = jax.random.uniform(jax.random.fold_in(jax.random.fold_in(own_key, 6), axis_at), (shards_of,), jnp.float32, least / len(shards), largest / len(shards))
        return jnp.repeat(jnp.exp(heights), shape[axis_at] // shards_of).reshape((-1,) + (1,) * (len(shape) - axis_at - 1))

    gain = one(*shards[0])
    for cut in shards[1:]:
        gain = gain * one(*cut)
    return gain


def shared_out(own_key, own, number, rows, number_of, top, limit, skew):
    ranking = jax.random.permutation(own_key, number_of)
    crowded, usual = load_shares(number_of, rows * top, limit, skew, True), load_shares(number_of, rows * top, limit, skew, False)
    places = jnp.arange(number_of)

    def named(tallies, turn):
        used = int((tallies > 0).sum())
        fixed = max(1, used // 4)
        moved = fixed + (places - fixed + turn * (used - fixed)) % max(1, number_of - fixed)
        return jnp.zeros((number_of,), jnp.int32).at[ranking[jnp.where(places < fixed, places, moved)]].set(jnp.asarray(tallies, jnp.int32))

    tallies = jnp.where(number % 4 == 0, named(crowded, number // 4), named(usual, number - number // 4 - 1))
    mixed = jax.random.permutation(jax.random.fold_in(own, 3), number_of)
    source_of, receiver = mixed[0:number_of // 2 * 2:2], mixed[1:number_of // 2 * 2:2]
    slack = jnp.minimum(tallies[source_of] - 1, limit - tallies[receiver]) // 2
    slack = jnp.where((source_of == ranking[0]) | (receiver == ranking[0]) | (tallies[receiver] == 0), 0, jnp.maximum(slack, 0))
    moved = jax.random.randint(jax.random.fold_in(own, 4), (number_of // 2,), 0, 1 << 20) % (slack + 1)
    tallies = tallies.at[source_of].add(-moved).at[receiver].add(moved)
    items = jnp.searchsorted(jnp.cumsum(tallies), jnp.arange(rows * top), side="right").astype(jnp.int32)
    table = items.reshape(top, rows).T
    table = table[jax.random.permutation(jax.random.fold_in(own, 1), rows)]
    turn = jax.random.randint(jax.random.fold_in(own, 2), (rows, 1), 0, top)
    return jnp.take_along_axis(table, (jnp.arange(top)[None, :] + turn) % top, axis=1)


def load_shares(count, total, most, skew, full):
    portions = [(1 << 20) // math.isqrt(grade ** skew) + 1 for grade in range(1, count + 1)]
    largest = most if full else min(most, max(-(-total // count), total * portions[0] // sum(portions)))
    least = 1 if total - largest >= count - 1 else 0
    given, rest = [largest] + [least] * (count - 1), total - largest - least * (count - 1)
    while rest > 0:
        candidates = [i for i in range(1, count) if given[i] < largest] or [i for i in range(1, count) if given[i] < most]
        whole, budget = sum([portions[i] for i in candidates]), rest
        for i in candidates:
            extra = min(most - given[i], max(1, budget * portions[i] // whole), rest)
            given[i] = given[i] + extra
            rest = rest - extra
    return np.array(given)


def scatter_about(stream_key, extent, deviation, most, cuts=(), held_as=jnp.bfloat16):
    array = deviation * jax.random.normal(stream_key, extent, jnp.float32)
    if cuts:
        array = array * levels(stream_key, extent, cuts, -0.22, 0.18)
    return jnp.clip(array, -most, most).astype(held_as)


def setup_inputs(seed: int = 0) -> dict:
    key_list = jax.random.split(jax.random.key(seed), 7)
    tokens = scatter_about(key_list[0], (TOKENS, D), 1.0, 6.0, ((0, 16),))
    expert_ids_keys = jax.random.split(jax.random.fold_in(key_list[1], 1), TOKENS // TOK_DEV)
    expert_ids_turns = jax.random.permutation(jax.random.fold_in(key_list[1], 3), TOKENS // TOK_DEV)
    expert_ids = jax.vmap(lambda own, number: shared_out(jax.random.fold_in(key_list[1], 2), own, number, TOK_DEV, EXPERTS, TOPK, CAP, 2))(expert_ids_keys, expert_ids_turns).reshape((TOKENS, TOPK))
    route_weight = jnp.clip(jnp.exp(math.log(0.5) - 2.3025851 * jax.random.uniform(key_list[2], (TOKENS, TOPK), jnp.float32) ** levels(key_list[2], (TOKENS, TOPK), ((0, 16),), -0.2, 0.2)), 0.05, 0.5)
    w_gate = scatter_about(key_list[3], (EXPERTS, D, FF), D ** -0.5, 0.09375, ((0, 16), (2, 2)))
    w_up = scatter_about(key_list[4], (EXPERTS, D, FF), D ** -0.5, 0.09375, ((0, 16), (2, 2)))
    w_down = scatter_about(key_list[5], (EXPERTS, FF, D), FF ** -0.5, 0.1875, ((0, 16), (1, 2)))
    return {"tokens": tokens, "expert_ids": expert_ids, "route_weight": route_weight, "w_gate": w_gate, "w_up": w_up, "w_down": w_down}


def reference(tokens, expert_ids, route_weight, w_gate, w_up, w_down):
    groups = N_ULY * N_DP
    model_width = tokens.shape[1]
    hidden_cut = FF // N_BLK
    grouped = tokens.reshape(groups, TOK_DEV, model_width)
    grouped_ids = expert_ids.reshape(groups, TOK_DEV, TOPK)
    weights = route_weight.reshape(groups, TOK_DEV, TOPK)
    labels = jnp.arange(EXPERTS, dtype=jnp.int32)
    onehot = (grouped_ids[:, :, :, None] == labels[None, None, None, :]).astype(jnp.int32)
    chosen = jnp.sum(onehot, axis=2)
    before = jnp.cumsum(chosen, axis=1) - chosen
    weight_share = jnp.sum(onehot.astype(route_weight.dtype) * weights[:, :, :, None], axis=2)
    positions = jnp.arange(TOK_DEV, dtype=jnp.int32)
    places = jnp.arange(CAP, dtype=jnp.int32)

    def one_expert(running, inputs):
        gate_matrix, up_matrix, down_matrix, picked, slot_rank, scaled = inputs
        matched = ((picked[:, :, None] == 1) & (slot_rank[:, :, None] == places[None, None, :])).astype(jnp.int32)
        source = jnp.sum(matched * positions[None, :, None], axis=1).astype(jnp.int32)
        filled = jnp.sum(matched, axis=1)
        index_full = jnp.broadcast_to(source[:, :, None], (groups, CAP, model_width)).astype(jnp.int32)
        selected = jnp.take_along_axis(grouped, index_full, axis=1)
        selected = jnp.where(filled[:, :, None] == 1, selected, jnp.zeros_like(selected))
        selected = selected.reshape(groups * CAP, model_width)
        gate_sum = jnp.dot(selected, gate_matrix, preferred_element_type=jnp.float32)
        up_sum = jnp.dot(selected, up_matrix, preferred_element_type=jnp.float32)
        hidden = (jax.nn.silu(gate_sum) * up_sum).astype(jnp.bfloat16)
        pieces = jnp.einsum("rbf,bfd->brd",
                            hidden.astype(jnp.float32).reshape(groups * CAP, N_BLK, hidden_cut),
                            down_matrix.astype(jnp.float32).reshape(N_BLK, hidden_cut, model_width))
        pieces = lax.optimization_barrier(pieces.astype(jnp.bfloat16)).astype(jnp.float32)
        answer = jnp.sum(pieces, axis=0).astype(jnp.bfloat16).reshape(groups, CAP, model_width)
        back_index = jnp.broadcast_to(jnp.clip(slot_rank, 0, CAP - 1)[:, :, None], (groups, TOK_DEV, model_width)).astype(jnp.int32)
        gathered = jnp.take_along_axis(answer, back_index, axis=1)
        return running + scaled[:, :, None] * gathered.astype(jnp.float32), None

    start_value = jnp.zeros((groups, TOK_DEV, model_width), jnp.float32)
    inputs = (w_gate, w_up, w_down,
              jnp.transpose(chosen, (2, 0, 1)),
              jnp.transpose(before, (2, 0, 1)),
              jnp.transpose(weight_share, (2, 0, 1)))
    running, _ = lax.scan(one_expert, start_value, inputs)
    return running.reshape(groups * TOK_DEV, model_width).astype(jnp.bfloat16)
```

```python
import jax
import jax.numpy as jnp
from jax import lax
from jax.sharding import PartitionSpec as P


def routing_tables(expert_ids, route_weight, groups, local_count, capacity):
    tokens_here, picks_count = expert_ids.shape
    experts = groups * local_count
    labels = lax.broadcasted_iota(jnp.int32, (1, 1, experts), 2)
    onehot = (expert_ids[:, :, None] == labels).astype(jnp.int32)
    chosen = jnp.sum(onehot, axis=1)
    before = jnp.cumsum(chosen, axis=0) - chosen
    slot_of = jnp.sum(onehot * before[:, None, :], axis=2)
    places = lax.broadcasted_iota(jnp.int32, (1, 1, capacity), 2)
    slot_hot = (slot_of[:, :, None] == places).astype(jnp.float32)
    expert_hot = onehot.astype(jnp.float32).reshape(tokens_here, picks_count, groups, local_count)
    placing = jnp.einsum("tkgl,tkc->gclt", expert_hot, slot_hot)
    placing = placing.reshape(groups * capacity * local_count, tokens_here)
    mixing = jnp.einsum("tkgl,tkc,tk->tgcl", expert_hot, slot_hot, route_weight)
    mixing = mixing.reshape(tokens_here, groups * capacity * local_count)
    return (placing.astype(jnp.bfloat16), mixing)


def local_slots(tokens, expert_ids, route_weight, w_gate, w_up, w_down):
    ulysses_size = lax.axis_size("uly")
    data_size = lax.axis_size("dp")
    cycle_size = lax.axis_size("blk")
    tokens_here, model_width = tokens.shape
    local_count = w_gate.shape[0]
    hidden_cut = w_gate.shape[2]
    groups = ulysses_size * data_size
    experts = groups * local_count
    picks_count = expert_ids.shape[1]
    capacity = min(tokens_here, max(2, 5 * tokens_here * picks_count // (4 * experts)))
    placing, mixing = routing_tables(expert_ids, route_weight, groups, local_count, capacity)
    slice_width = model_width // cycle_size
    rows_total = groups * capacity
    cycle_index = lax.axis_index("blk")
    own_part = lax.dynamic_slice_in_dim(tokens, cycle_index * slice_width, slice_width, 1)
    outgoing = jnp.dot(placing, own_part, preferred_element_type=jnp.float32).astype(jnp.bfloat16)
    outgoing = outgoing.reshape(ulysses_size, data_size, capacity, local_count, slice_width)
    arrived = lax.all_to_all(
        lax.all_to_all(outgoing, "uly", split_axis=0, concat_axis=0, tiled=True),
        "dp",
        split_axis=1,
        concat_axis=1,
        tiled=True,
    )
    arrived = arrived.reshape(rows_total, local_count, slice_width)
    portion = lax.all_gather(arrived, "blk", axis=2, tiled=True)
    gate_more = jnp.einsum("rlw,lwf->rlf", portion, w_gate, preferred_element_type=jnp.float32)
    up_more = jnp.einsum("rlw,lwf->rlf", portion, w_up, preferred_element_type=jnp.float32)
    hidden = (jax.nn.silu(gate_more) * up_more).astype(jnp.bfloat16)
    resplit = lax.all_to_all(w_down, "blk", split_axis=2, concat_axis=1, tiled=True)
    zero_sum = jnp.zeros((slice_width, rows_total * local_count), jnp.float32)
    total = zero_sum
    portion = lax.all_gather(hidden, "blk", axis=2, tiled=True)
    ranges_count = portion.shape[2] // hidden_cut
    for number in range(ranges_count):
        part_hidden = portion[:, :, number * hidden_cut : (number + 1) * hidden_cut]
        part_rows = lax.dynamic_slice_in_dim(resplit, number * hidden_cut, hidden_cut, 1)
        partial_value = jnp.einsum(
            "lfd,rlf->drl", part_rows, part_hidden, preferred_element_type=jnp.float32
        )
        partial_value = partial_value.reshape(slice_width, rows_total * local_count)
        total = total + partial_value.astype(jnp.bfloat16).astype(jnp.float32)
    returned = total.astype(jnp.bfloat16).reshape(
        slice_width, ulysses_size, data_size, capacity, local_count
    )
    returned_rows = lax.all_to_all(
        lax.all_to_all(returned, "uly", split_axis=1, concat_axis=1, tiled=True),
        "dp",
        split_axis=2,
        concat_axis=2,
        tiled=True,
    )
    returned_rows = returned_rows.reshape(slice_width, rows_total * local_count).astype(jnp.float32)
    mixed = lax.dot_general(
        mixing, returned_rows, (((1,), (1,)), ((), ())), precision=lax.Precision.HIGHEST
    )
    return mixed.astype(jnp.bfloat16)


def local_dense(tokens, expert_ids, route_weight, w_gate, w_up, w_down):
    data_size = lax.axis_size("dp")
    local_count = w_gate.shape[0]
    groups = lax.axis_size("uly") * data_size
    experts = groups * local_count
    labels = lax.broadcasted_iota(jnp.int32, (1, 1, experts), 2)
    scaled = jnp.sum(jnp.where(expert_ids[:, :, None] == labels, route_weight[:, :, None], 0.0), axis=1)
    everyone = lax.all_gather(tokens, ("uly", "dp"), axis=0, tiled=True)
    shares = lax.all_gather(scaled, ("uly", "dp"), axis=0, tiled=True)
    first = (lax.axis_index("uly") * data_size + lax.axis_index("dp")) * local_count
    total = None
    for number in range(local_count):
        share = lax.dynamic_slice_in_dim(shares, first + number, 1, 1)
        gate = jnp.dot(everyone, w_gate[number], preferred_element_type=jnp.float32)
        up = jnp.dot(everyone, w_up[number], preferred_element_type=jnp.float32)
        hidden = (jax.nn.silu(gate) * up * share).astype(jnp.bfloat16)
        part = jnp.dot(hidden, w_down[number], preferred_element_type=jnp.float32)
        total = part if total is None else total + part
    halves = lax.psum_scatter(total.astype(jnp.bfloat16), "blk", scatter_dimension=1, tiled=True)
    return lax.psum_scatter(halves, ("uly", "dp"), scatter_dimension=0, tiled=True)


def solution(mesh):
    groups = mesh.shape["uly"] * mesh.shape["dp"]
    return jax.shard_map(
        local_dense if groups <= 16 else local_slots,
        mesh=mesh,
        in_specs=(
            P(("uly", "dp"), None),
            P(("uly", "dp"), None),
            P(("uly", "dp"), None),
            P(("uly", "dp"), None, "blk"),
            P(("uly", "dp"), None, "blk"),
            P(("uly", "dp"), "blk", None),
        ),
        out_specs=P(("uly", "dp"), "blk"),
        check_vma=False,
    )
```

```python
import jax
import jax.numpy as jnp
from jax import lax
from jax.experimental import pallas as pl
from jax.experimental.pallas import tpu as pltpu
from jax.sharding import PartitionSpec as P


def routing_tables(expert_ids, route_weight, groups, local_count, capacity):
    tokens_here, picks_count = expert_ids.shape
    experts = groups * local_count
    labels = lax.broadcasted_iota(jnp.int32, (1, 1, experts), 2)
    onehot = (expert_ids[:, :, None] == labels).astype(jnp.int32)
    chosen = jnp.sum(onehot, axis=1)
    before = jnp.cumsum(chosen, axis=0) - chosen
    slot_of = jnp.sum(onehot * before[:, None, :], axis=2)
    places = lax.broadcasted_iota(jnp.int32, (1, 1, capacity), 2)
    slot_hot = (slot_of[:, :, None] == places).astype(jnp.float32)
    expert_hot = onehot.astype(jnp.float32).reshape(tokens_here, picks_count, groups, local_count)
    placing = jnp.einsum("tkgl,tkc->gclt", expert_hot, slot_hot)
    placing = placing.reshape(groups * capacity * local_count, tokens_here)
    mixing = jnp.einsum("tkgl,tkc,tk->tgcl", expert_hot, slot_hot, route_weight)
    mixing = mixing.reshape(tokens_here, groups * capacity * local_count)
    return (placing.astype(jnp.bfloat16), mixing)


def local_slots(tokens, expert_ids, route_weight, w_gate, w_up, w_down):
    ulysses_size = lax.axis_size("uly")
    data_size = lax.axis_size("dp")
    cycle_size = lax.axis_size("blk")
    tokens_here, model_width = tokens.shape
    local_count = w_gate.shape[0]
    hidden_cut = w_gate.shape[2]
    groups = ulysses_size * data_size
    experts = groups * local_count
    picks_count = expert_ids.shape[1]
    capacity = min(tokens_here, max(2, 5 * tokens_here * picks_count // (4 * experts)))
    placing, mixing = routing_tables(expert_ids, route_weight, groups, local_count, capacity)
    slice_width = model_width // cycle_size
    rows_total = groups * capacity
    cycle_index = lax.axis_index("blk")
    own_part = lax.dynamic_slice_in_dim(tokens, cycle_index * slice_width, slice_width, 1)
    outgoing = jnp.dot(placing, own_part, preferred_element_type=jnp.float32).astype(jnp.bfloat16)
    outgoing = outgoing.reshape(ulysses_size, data_size, capacity, local_count, slice_width)
    arrived = lax.all_to_all(
        lax.all_to_all(outgoing, "uly", split_axis=0, concat_axis=0, tiled=True),
        "dp",
        split_axis=1,
        concat_axis=1,
        tiled=True,
    )
    arrived = arrived.reshape(rows_total, local_count, slice_width)
    portion = lax.all_gather(arrived, "blk", axis=2, tiled=True)
    gate_more = jnp.einsum("rlw,lwf->rlf", portion, w_gate, preferred_element_type=jnp.float32)
    up_more = jnp.einsum("rlw,lwf->rlf", portion, w_up, preferred_element_type=jnp.float32)
    hidden = (jax.nn.silu(gate_more) * up_more).astype(jnp.bfloat16)
    resplit = lax.all_to_all(w_down, "blk", split_axis=2, concat_axis=1, tiled=True)
    zero_sum = jnp.zeros((slice_width, rows_total * local_count), jnp.float32)
    total = zero_sum
    portion = lax.all_gather(hidden, "blk", axis=2, tiled=True)
    ranges_count = portion.shape[2] // hidden_cut
    for number in range(ranges_count):
        part_hidden = portion[:, :, number * hidden_cut : (number + 1) * hidden_cut]
        part_rows = lax.dynamic_slice_in_dim(resplit, number * hidden_cut, hidden_cut, 1)
        partial_value = jnp.einsum(
            "lfd,rlf->drl", part_rows, part_hidden, preferred_element_type=jnp.float32
        )
        partial_value = partial_value.reshape(slice_width, rows_total * local_count)
        total = total + partial_value.astype(jnp.bfloat16).astype(jnp.float32)
    returned = total.astype(jnp.bfloat16).reshape(
        slice_width, ulysses_size, data_size, capacity, local_count
    )
    returned_rows = lax.all_to_all(
        lax.all_to_all(returned, "uly", split_axis=1, concat_axis=1, tiled=True),
        "dp",
        split_axis=2,
        concat_axis=2,
        tiled=True,
    )
    returned_rows = returned_rows.reshape(slice_width, rows_total * local_count).astype(jnp.float32)
    mixed = lax.dot_general(
        mixing, returned_rows, (((1,), (1,)), ((), ())), precision=lax.Precision.HIGHEST
    )
    return mixed.astype(jnp.bfloat16)


MESH = pl.DeviceIdType.MESH


def neighbours(deep):
    at_y, at_u, at_z = lax.axis_index("blk"), lax.axis_index("uly"), lax.axis_index("dp")
    at_x, core = at_u // 2, at_u % 2
    devices = {
        "up": {"dp": jnp.minimum(at_z + 1, deep - 1)},
        "down": {"dp": jnp.maximum(at_z - 1, 0)},
        "x": {"uly": (1 - at_x) * 2 + core},
        "y": {"blk": 1 - at_y},
        "core": {"uly": at_x * 2 + 1 - core},
    }
    return at_x, at_y, at_z, core, devices


def greet(deep, at_z, devices):
    barrier = pltpu.get_barrier_semaphore()
    for name in ("x", "y", "core"):
        pl.semaphore_signal(barrier, inc=1, device_id=devices[name], device_id_type=MESH)

    @pl.when(at_z > 0)
    def _():
        pl.semaphore_signal(barrier, inc=1, device_id=devices["down"], device_id_type=MESH)

    @pl.when(at_z < deep - 1)
    def _():
        pl.semaphore_signal(barrier, inc=1, device_id=devices["up"], device_id_type=MESH)

    beside = (at_z > 0).astype(jnp.int32) + (at_z < deep - 1).astype(jnp.int32)
    pl.semaphore_wait(barrier, 3 + beside)


def gather_kernel(deep, parts, apart, tok, own_share, every, shares, own_sem, send, recv):
    at_x, at_y, at_z, core, devices = neighbours(deep)
    rows_each, width = tok.shape
    piece = rows_each // parts
    plane = width - apart
    plane_cols = pl.ds(pl.multiple_of(at_y * apart, 128), plane)
    theirs = pl.ds(pl.multiple_of(at_y * plane, 128), apart)
    lacking = pl.ds(pl.multiple_of((1 - at_y) * plane, 128), apart)
    entire = pl.ds(0, width)
    pending = []

    def group(x_of, core_of, z_of):
        return (2 * x_of + core_of) * deep + z_of

    def block(x_of, core_of, z_of, k, cols):
        start = pl.multiple_of(group(x_of, core_of, z_of) * rows_each + k * piece, piece)
        return every.at[pl.ds(start, piece), cols]

    def copy(src, dst, kind, index, to):
        return pltpu.make_async_remote_copy(
            src_ref=src, dst_ref=dst, send_sem=send.at[kind, index], recv_sem=recv.at[kind, index],
            device_id=devices[to], device_id_type=MESH)

    def start(condition, src, dst, kind, index, to):
        def go():
            copy(src, dst, kind, index, to).start()

        if condition is None:
            go()
        else:
            pl.when(condition)(go)
        pending.append((condition, src, dst, kind, index, to))

    def arrive(dst, kind, index):
        copy(dst, dst, kind, index, "x").wait_recv()

    greet(deep, at_z, devices)
    low, high = at_z > 0, at_z < deep - 1
    mine_at = pl.multiple_of(group(at_x, core, at_z) * rows_each, rows_each)
    placed = pltpu.make_async_copy(tok, every.at[pl.ds(mine_at, rows_each)], own_sem.at[0])
    placed.start()
    share_at = shares.at[group(at_x, core, at_z)]
    share_placed = pltpu.make_async_copy(own_share, share_at, own_sem.at[1])
    share_placed.start()
    for k in range(parts):
        here = at_z * parts + k
        source = tok.at[pl.ds(k * piece, piece), plane_cols]
        target = block(at_x, core, at_z, k, plane_cols)
        start(high, source, target, 0, here, "up")
        start(low, source, target, 1, here, "down")
        start(None, source, target, 2, here, "x")
    start(high, own_share, share_at, 9, at_z, "up")
    start(low, own_share, share_at, 10, at_z, "down")
    start(None, own_share, share_at, 11, at_z, "x")
    for k in range(parts):
        start(None, tok.at[pl.ds(k * piece, piece)], block(at_x, core, at_z, k, entire), 5, at_z * parts + k, "core")
    start(None, own_share, share_at, 12, at_z, "core")

    def from_z(condition, onward, kind, to, z_of, k):
        held = block(at_x, core, z_of, k, plane_cols)
        index = z_of * parts + k
        pl.when(condition)(lambda: arrive(held, kind, index))
        start(condition & onward, held, held, kind, index, to)
        start(condition, held, held, 2, index, "x")
        sent = block(at_x, core, z_of, k, theirs)
        start(condition, sent, sent, 3, index, "y")
        start(condition, held, held, 5, index, "core")
        if k == parts - 1:
            share = shares.at[group(at_x, core, z_of)]
            pl.when(condition)(lambda: arrive(share, kind + 9, z_of))
            start(condition & onward, share, share, kind + 9, z_of, to)
            start(condition, share, share, 11, z_of, "x")
            start(condition, share, share, 12, z_of, "core")

    def from_x(condition, z_of, k):
        held = block(1 - at_x, core, z_of, k, plane_cols)
        index = z_of * parts + k
        sent = block(1 - at_x, core, z_of, k, theirs)
        pl.when(condition)(lambda: arrive(held, 2, index))
        start(condition, sent, sent, 4, index, "y")
        start(condition, held, held, 6, index, "core")
        if k == parts - 1:
            share = shares.at[group(1 - at_x, core, z_of)]
            pl.when(condition)(lambda: arrive(share, 11, z_of))
            start(condition, share, share, 13, z_of, "core")

    def below(step):
        return at_z >= step, jnp.maximum(at_z - step, 0)

    def above(step):
        return at_z + step < deep, jnp.minimum(at_z + step, deep - 1)

    def sides(step):
        return [(at_z >= 0, at_z)] if step == 0 else [below(step), above(step)]

    for step in range(1, deep + 1):
        for k in range(parts):
            if step < deep:
                there, z_of = below(step)
                from_z(there, high, 0, "up", z_of, k)
                there, z_of = above(step)
                from_z(there, low, 1, "down", z_of, k)
            for there, z_of in sides(step - 1):
                from_x(there, z_of, k)

    def from_y(condition, x_of, kind, z_of, k):
        held = block(x_of, core, z_of, k, lacking)
        index = z_of * parts + k
        pl.when(condition)(lambda: arrive(held, kind, index))
        start(condition, held, held, kind + 4, index, "core")

    def each_remote(act):
        for step in range(deep):
            for k in range(parts):
                for there, z_of in sides(step):
                    if step > 0:
                        act(there, at_x, 3, z_of, k)
                    act(there, 1 - at_x, 4, z_of, k)

    each_remote(from_y)

    def from_core(condition, x_of, kind, z_of, k):
        index = z_of * parts + k

        @pl.when(condition)
        def _():
            arrive(block(x_of, 1 - core, z_of, k, plane_cols), kind + 2, index)
            arrive(block(x_of, 1 - core, z_of, k, lacking), kind + 4, index)
            if k == parts - 1:
                arrive(shares.at[group(x_of, 1 - core, z_of)], kind + 9, z_of)

    for k in range(parts):
        arrive(block(at_x, 1 - core, at_z, k, entire), 5, at_z * parts + k)
    arrive(shares.at[group(at_x, 1 - core, at_z)], 12, at_z)
    each_remote(from_core)
    placed.wait()
    share_placed.wait()
    for condition, src, dst, kind, index, to in pending:
        def end(src=src, dst=dst, kind=kind, index=index, to=to):
            copy(src, dst, kind, index, to).wait_send()

        if condition is None:
            end()
        else:
            pl.when(condition)(end)


def gather(tokens, share, groups, deep):
    rows_each, width = tokens.shape
    parts = 2
    apart = width * 3 // 8 // 128 * 128
    vmem = pl.BlockSpec(memory_space=pltpu.VMEM)
    return pl.pallas_call(
        lambda *refs: gather_kernel(deep, parts, apart, *refs),
        out_shape=(
            jax.ShapeDtypeStruct((groups * rows_each, width), tokens.dtype),
            jax.ShapeDtypeStruct((groups,) + share.shape, share.dtype),
        ),
        in_specs=[vmem, vmem],
        out_specs=(vmem, vmem),
        scratch_shapes=[
            pltpu.SemaphoreType.DMA((2,)),
            pltpu.SemaphoreType.DMA((14, deep * parts)),
            pltpu.SemaphoreType.DMA((14, deep * parts)),
        ],
        compiler_params=pltpu.CompilerParams(
            collective_id=0, has_side_effects=True, vmem_limit_bytes=40 << 20),
    )(tokens, share)


def scatter_kernel(deep, low_half, high_half, out, total, a1, a2, b1, b2, rising, falling, send, recv):
    at_x, at_y, at_z, core, devices = neighbours(deep)
    rows_each = out.shape[0]
    part = rows_each // 2
    halves = (low_half, high_half)
    pending = []
    order = []
    for number in range((deep + 1) // 2):
        order += [number] if number == deep - 1 - number else [number, deep - 1 - number]

    def copy(src, dst, kind, index, to):
        return pltpu.make_async_remote_copy(
            src_ref=src, dst_ref=dst, send_sem=send.at[kind, index], recv_sem=recv.at[kind, index],
            device_id=devices[to], device_id_type=MESH)

    def start(condition, *what):
        def go():
            copy(*what).start()

        if condition is None:
            go()
        else:
            pl.when(condition)(go)
        pending.append((condition, what))

    def rows_of(x_of, core_of, z_of):
        first = ((2 * x_of + core_of) * deep + z_of) * rows_each
        return pl.ds(pl.multiple_of(first, rows_each), rows_each)

    def added(one, other):
        return (one.astype(jnp.float32) + other.astype(jnp.float32)).astype(jnp.bfloat16)

    greet(deep, at_z, devices)
    for z_of in order:
        for x_of in range(2):
            for half in range(2):
                start(None, halves[half].at[rows_of(x_of, 1 - core, z_of)], total.at[z_of, x_of, half],
                      0, (z_of * 2 + x_of) * 2 + half, "core")
    upper, lower = pl.ds(0, part), pl.ds(part, part)
    for z_of in order:
        for x_of in range(2):
            for half in range(2):
                spot = total.at[z_of, x_of, half]
                copy(spot, spot, 0, (z_of * 2 + x_of) * 2 + half, "core").wait_recv()
                total[z_of, x_of, half] = added(total[z_of, x_of, half], halves[half][rows_of(x_of, core, z_of), :])
        start(None, total.at[z_of, :, 1 - at_y, upper], a1.at[z_of], 1, z_of, "y")
        start(None, total.at[z_of, 1 - at_x, :, lower], b1.at[z_of], 2, z_of, "x")

    def first_stage(z_of):
        copy(a1.at[z_of], a1.at[z_of], 1, z_of, "y").wait_recv()
        for x_of in range(2):
            total[z_of, x_of, at_y, upper] = added(total[z_of, x_of, at_y, upper], a1[z_of, x_of])
        start(None, total.at[z_of, 1 - at_x, at_y, upper], a2.at[z_of], 3, z_of, "x")
        copy(b1.at[z_of], b1.at[z_of], 2, z_of, "x").wait_recv()
        for half in range(2):
            total[z_of, at_x, half, lower] = added(total[z_of, at_x, half, lower], b1[z_of, half])
        start(None, total.at[z_of, at_x, 1 - at_y, lower], b2.at[z_of], 4, z_of, "y")

    def second_stage(z_of):
        copy(a2.at[z_of], a2.at[z_of], 3, z_of, "x").wait_recv()
        total[z_of, at_x, at_y, upper] = added(total[z_of, at_x, at_y, upper], a2[z_of])
        copy(b2.at[z_of], b2.at[z_of], 4, z_of, "y").wait_recv()
        total[z_of, at_x, at_y, lower] = added(total[z_of, at_x, at_y, lower], b2[z_of])

    def third_stage(z_of):
        for toward, farther, inbound, kind, to in (
            (at_z < z_of, at_z > 0, rising, 5, "up"),
            (at_z > z_of, at_z < deep - 1, falling, 6, "down"),
        ):
            @pl.when(toward & farther)
            def _(inbound=inbound, kind=kind, to=to):
                copy(inbound.at[z_of], inbound.at[z_of], kind, z_of, to).wait_recv()
                total[z_of, at_x, at_y] = added(total[z_of, at_x, at_y], inbound[z_of])

            start(toward, total.at[z_of, at_x, at_y], inbound.at[z_of], kind, z_of, to)

    for number in range(deep + 2):
        if number < deep:
            first_stage(order[number])
        if 0 <= number - 1 < deep:
            second_stage(order[number - 1])
        if 0 <= number - 2 < deep:
            third_stage(order[number - 2])

    @pl.when(at_z > 0)
    def _():
        copy(rising.at[at_z], rising.at[at_z], 5, at_z, "up").wait_recv()
        total[at_z, at_x, at_y] = added(total[at_z, at_x, at_y], rising[at_z])

    @pl.when(at_z < deep - 1)
    def _():
        copy(falling.at[at_z], falling.at[at_z], 6, at_z, "down").wait_recv()
        total[at_z, at_x, at_y] = added(total[at_z, at_x, at_y], falling[at_z])

    out[...] = total[at_z, at_x, at_y]
    for condition, what in pending:
        def end(what=what):
            copy(*what).wait_send()

        if condition is None:
            end()
        else:
            pl.when(condition)(end)


def scatter(low_half, high_half, rows_each, deep):
    width = low_half.shape[1]
    part = rows_each // 2
    kind = low_half.dtype
    vmem = pl.BlockSpec(memory_space=pltpu.VMEM)
    return pl.pallas_call(
        lambda *refs: scatter_kernel(deep, *refs),
        out_shape=jax.ShapeDtypeStruct((rows_each, width), kind),
        in_specs=[vmem, vmem],
        out_specs=vmem,
        scratch_shapes=[
            pltpu.VMEM((deep, 2, 2, rows_each, width), kind),
            pltpu.VMEM((deep, 2, part, width), kind),
            pltpu.VMEM((deep, part, width), kind),
            pltpu.VMEM((deep, 2, part, width), kind),
            pltpu.VMEM((deep, part, width), kind),
            pltpu.VMEM((deep, rows_each, width), kind),
            pltpu.VMEM((deep, rows_each, width), kind),
            pltpu.SemaphoreType.DMA((7, deep * 4)),
            pltpu.SemaphoreType.DMA((7, deep * 4)),
        ],
        compiler_params=pltpu.CompilerParams(
            collective_id=1, has_side_effects=True, vmem_limit_bytes=48 << 20),
    )(low_half, high_half)


def local_dense(tokens, expert_ids, route_weight, w_gate, w_up, w_down):
    deep = lax.axis_size("dp")
    groups = lax.axis_size("uly") * deep
    rows_each = tokens.shape[0]
    labels = lax.broadcasted_iota(jnp.int32, (groups, 1, 1), 0)
    scaled = jnp.sum(jnp.where(expert_ids[None] == labels, route_weight[None], 0.0), axis=2)
    scaled = jnp.pad(scaled, ((0, 0), (0, -rows_each % 128)))
    everyone, shares = gather(tokens, scaled, groups, deep)
    first = lax.axis_index("uly") * deep + lax.axis_index("dp")
    share = lax.dynamic_slice_in_dim(shares, first, 1, 1)[:, 0, :rows_each].reshape(groups * rows_each, 1)
    gate = jnp.dot(everyone, w_gate[0], preferred_element_type=jnp.float32)
    up = jnp.dot(everyone, w_up[0], preferred_element_type=jnp.float32)
    hidden = (jax.nn.silu(gate) * up * share).astype(jnp.bfloat16)
    half = w_down.shape[2] // 2
    low_half = jnp.dot(hidden, w_down[0, :, :half], preferred_element_type=jnp.float32).astype(jnp.bfloat16)
    high_half = jnp.dot(hidden, w_down[0, :, half:], preferred_element_type=jnp.float32).astype(jnp.bfloat16)
    return scatter(low_half, high_half, rows_each, deep)


def solution(mesh):
    groups = mesh.shape["uly"] * mesh.shape["dp"]
    dense = mesh.shape["blk"] == 2 and mesh.shape["uly"] == 4 and groups <= 16
    return jax.shard_map(
        local_dense if dense else local_slots,
        mesh=mesh,
        in_specs=(
            P(("uly", "dp"), None),
            P(("uly", "dp"), None),
            P(("uly", "dp"), None),
            P(("uly", "dp"), None, "blk"),
            P(("uly", "dp"), None, "blk"),
            P(("uly", "dp"), "blk", None),
        ),
        out_specs=P(("uly", "dp"), "blk"),
        check_vma=False,
    )
```
